32 devices in a mesh: dp: 4 (over x, core), seq: 8 (over z, y).
Axes of the slice: x: 2, y: 2, z: 4, core: 2. Of those that a mesh axis runs over, the one named last changes fastest.
Arguments:
- tokens: bfloat16 [8, 1152, 1280], P('dp', 'seq'), may hold values from -60 to 60
- pre_gain: float32 [1280], replicated, may hold values from 0.5 to 1.5
- pre_shift: float32 [1280], replicated, may hold values from -3 to 3
- w_qkv: bfloat16 [1280, 3840], P('dp'), may hold values from -4 to 4
- qkv_bias: float32 [3840], replicated, may hold values from -3 to 3
- w_out: bfloat16 [1280, 1280], P('dp'), may hold values from -0.15625 to 0.15625
- out_bias: float32 [1280], replicated, may hold values from -3 to 3
- mlp_gain: float32 [1280], replicated, may hold values from 0.5 to 1.5
- mlp_shift: float32 [1280], replicated, may hold values from -3 to 3
- w_up: bfloat16 [1280, 2560], P('dp'), may hold values from -0.15625 to 0.15625
- up_bias: float32 [2560], replicated, may hold values from -3 to 3
- w_down: bfloat16 [2560, 1280], P('dp'), may hold values from -0.125 to 0.125
- down_bias: float32 [1280], replicated, may hold values from -3 to 3
Outputs:
- layer_out: bfloat16 [8, 1152, 1280], P('dp', 'seq')
The draws below stay inside these ranges and needn't reach their ends.
All inputs are finite; a program needn't handle non-finite values.
Results may differ from the reference program's by a relative error of at most 0.0039.
Values may be sent and summed in bfloat16 or wider, within the bound.
A program may use at most 128 MiB of HBM per device.

```python
import math
import jax
import jax.numpy as jnp
from jax import lax

D = 1280
HEADS = 16
HEAD_DIM = 80
FF = 2560
IMAGES = 8
SEQ_LEN = 1152


def draw_tokens(key, part):
    subkeys = jax.random.split(jax.random.fold_in(key, 21), 4)
    shape = (IMAGES, SEQ_LEN, D)
    base = jax.random.normal(subkeys[0], shape, jnp.float32)
    row_scale = jnp.exp(jax.random.uniform(subkeys[2], (IMAGES, SEQ_LEN, 1), jnp.float32, math.log(0.4), math.log(4.0)))
    col_scale = jnp.exp(jax.random.uniform(subkeys[3], (1, 1, D), jnp.float32, math.log(0.4), math.log(4.0)))
    values = base * row_scale * col_scale
    return jnp.clip(values, -60.0, 60.0).astype(jnp.bfloat16)


def draw_w_qkv(key, part):
    subkey = jax.random.fold_in(key, 33)
    shape = (D, 3 * D)
    values = jnp.clip(jax.random.normal(subkey, shape, jnp.float32), -6.0, 6.0) / math.sqrt(D)
    return values.astype(jnp.bfloat16)


def block_levels(stream_key, extent, cuts, smallest, top_value):
    def one(axis_at, blocks):
        steps = jax.random.uniform(jax.random.fold_in(jax.random.fold_in(stream_key, 6), axis_at), (blocks,), jnp.float32, smallest / len(cuts), top_value / len(cuts))
        return jnp.repeat(jnp.exp(steps), extent[axis_at] // blocks).reshape((-1,) + (1,) * (len(extent) - axis_at - 1))

    level = one(*cuts[0])
    for cut in cuts[1:]:
        level = level * one(*cut)
    return level


def bell_draw(stream_key, extent, deviation, bound, cuts=(), held_as=jnp.bfloat16):
    array = jax.random.normal(stream_key, extent, jnp.float32) * deviation
    if len(cuts) > 0:
        array = block_levels(stream_key, extent, cuts, -0.22, 0.18) * array
    return jnp.clip(array, min=-bound, max=bound).astype(held_as)


def setup_inputs(seed: int = 0) -> dict:
    key_of = jax.random.split(jax.random.key(seed), 14)
    return {
        "tokens": draw_tokens(jax.random.fold_in(key_of[13], 71), 0),
        "pre_gain": jnp.clip(1.0 + 0.1 * jax.random.normal(key_of[1], (D,), jnp.float32), 0.5, 1.5),
        "pre_shift": bell_draw(key_of[2], (D,), 0.5, 3.0, (), jnp.float32),
        "w_qkv": draw_w_qkv(jax.random.fold_in(key_of[13], 71), 0),
        "qkv_bias": bell_draw(key_of[4], (3 * D,), 0.5, 3.0, (), jnp.float32),
        "w_out": bell_draw(key_of[5], (D, D), D ** -0.5, 0.15625, ((0, 4),)),
        "out_bias": bell_draw(key_of[6], (D,), 0.5, 3.0, (), jnp.float32),
        "mlp_gain": jnp.clip(1.0 + 0.1 * jax.random.normal(key_of[7], (D,), jnp.float32), 0.5, 1.5),
        "mlp_shift": bell_draw(key_of[8], (D,), 0.5, 3.0, (), jnp.float32),
        "w_up": bell_draw(key_of[9], (D, FF), D ** -0.5, 0.15625, ((0, 4),)),
        "up_bias": bell_draw(key_of[10], (FF,), 0.5, 3.0, (), jnp.float32),
        "w_down": bell_draw(key_of[11], (FF, D), FF ** -0.5, 0.125, ((0, 4),)),
        "down_bias": bell_draw(key_of[12], (D,), 0.5, 3.0, (), jnp.float32),
    }


EPSILON = 1e-05

def normalize(features, gain, shift):
    average = lax.optimization_barrier(jnp.mean(features, axis=-1, keepdims=True))
    centered = features - average
    spread = lax.optimization_barrier(jnp.mean(centered * centered, axis=-1, keepdims=True))
    return centered * lax.rsqrt(spread + EPSILON) * gain + shift

def attend_head(packed_head):
    queries = packed_head[:, :HEAD_DIM]
    key_rows = packed_head[:, HEAD_DIM:2 * HEAD_DIM]
    value_rows = packed_head[:, 2 * HEAD_DIM:]
    scores = jnp.dot(queries, key_rows.T, preferred_element_type=jnp.float32) * (1.0 / math.sqrt(HEAD_DIM))
    highest = lax.optimization_barrier(jnp.max(scores, axis=-1, keepdims=True))
    weights = jnp.exp(scores - highest)
    probs = (weights / lax.optimization_barrier(jnp.sum(weights, axis=-1, keepdims=True))).astype(jnp.bfloat16)
    return jnp.dot(probs, value_rows, preferred_element_type=jnp.float32).astype(jnp.bfloat16)

def reference(tokens, pre_gain, pre_shift, w_qkv, qkv_bias, w_out, out_bias, mlp_gain, mlp_shift, w_up, up_bias, w_down, down_bias):

    def one_picture(picture):
        residual = picture.astype(jnp.float32)
        normed = normalize(residual, pre_gain, pre_shift).astype(jnp.bfloat16)
        packed = (jnp.dot(normed, w_qkv, preferred_element_type=jnp.float32) + qkv_bias).astype(jnp.bfloat16)
        per_head = packed.reshape(SEQ_LEN, HEADS, 3 * HEAD_DIM).transpose(1, 0, 2)
        context = lax.map(attend_head, per_head)
        context = context.transpose(1, 0, 2).reshape(SEQ_LEN, D)
        middle = residual + jnp.dot(context, w_out, preferred_element_type=jnp.float32) + out_bias
        normed_mlp = normalize(middle, mlp_gain, mlp_shift).astype(jnp.bfloat16)
        lifted = jnp.dot(normed_mlp, w_up, preferred_element_type=jnp.float32) + up_bias
        hidden = jax.nn.gelu(lifted, approximate=False).astype(jnp.bfloat16)
        lowered = jnp.dot(hidden, w_down, preferred_element_type=jnp.float32)
        return (middle + lowered + down_bias).astype(jnp.bfloat16)
    return lax.map(one_picture, tokens)
```

```python
import functools
import math

import jax
import jax.numpy as jnp
from jax import lax
from jax.experimental import pallas as pl
from jax.experimental.pallas import tpu as pltpu
from jax.sharding import PartitionSpec as P

HEADS = 16
HEAD_DIM = 80
LANES = 128
EPSILON = 1e-05
MESH = pl.DeviceIdType.MESH
VMEM = pl.BlockSpec(memory_space=pltpu.VMEM)


def normalize(features, gain, shift):
    average = jnp.mean(features, axis=-1, keepdims=True)
    centered = features - average
    spread = jnp.mean(centered * centered, axis=-1, keepdims=True)
    return centered * lax.rsqrt(spread + EPSILON) * gain + shift


def fold_rows(left_side, shard_piece):
    return jnp.dot(left_side, shard_piece, preferred_element_type=jnp.float32)


def ring_to_seq(place, n):
    back = place // (n // 2)
    return (1 - back) * 2 * place + back * (2 * (n - 1 - place) + 1)


def seq_to_ring(s, n):
    odd = s % 2
    return (1 - odd) * (s // 2) + odd * (n - 1 - s // 2)


def project_kernel(
    n, n_dp, x_ref, w_ref, b_ref, out_ref, buf, wbuf, tok_send, tok_recv, w_send, w_recv, f_send, f_recv
):
    d, s = lax.axis_index("dp"), lax.axis_index("seq")
    place = seq_to_ring(s, n)
    right = ring_to_seq((place + 1) % n, n)
    left = ring_to_seq((place + n - 1) % n, n)
    sibling = d + 1 - 2 * (d % 2)
    rows = x_ref.shape[0]
    half = rows // 2
    depth = w_ref.shape[0]
    images, length, _ = out_ref.shape
    tok = rows // images
    steps = n // 2
    pairs = n_dp // 2

    barrier = pltpu.get_barrier_semaphore()
    for target in (right, left):
        pl.semaphore_signal(barrier, inc=1, device_id=(d, target), device_id_type=MESH)
    for j in range(1, pairs):
        pl.semaphore_signal(barrier, inc=1, device_id=((d + 2 * j) % n_dp, s), device_id_type=MESH)
    pl.semaphore_signal(barrier, inc=1, device_id=(sibling, s), device_id_type=MESH)
    pl.semaphore_wait(barrier, 2 + pairs)

    def token_copy(way, t, h, arriving=False):
        back = t + 1 if arriving else t
        origin = (place + n - back) % n if way == 0 else (place + back) % n
        part = pl.ds(h * half, half)
        here = buf.at[origin, part]
        return pltpu.make_async_remote_copy(
            src_ref=x_ref.at[part] if (t == 0 and not arriving) else here,
            dst_ref=here,
            send_sem=tok_send.at[way, t, h],
            recv_sem=tok_recv.at[way, t, h],
            device_id=(d, right if way == 0 else left),
            device_id_type=MESH,
        )

    def slab(owner):
        return pl.ds(pl.multiple_of(owner * depth, 16), depth)

    def w_copy(j, arriving=False):
        owner = (d + n_dp - 2 * j) % n_dp if arriving else d
        return pltpu.make_async_remote_copy(
            src_ref=w_ref,
            dst_ref=wbuf.at[slab(owner)],
            send_sem=w_send.at[j],
            recv_sem=w_recv.at[j],
            device_id=((d + 2 * j) % n_dp, s),
            device_id_type=MESH,
        )

    def f_copy(j, arriving=False):
        base = sibling if arriving else d
        owner = (base + n_dp - 2 * j) % n_dp
        return pltpu.make_async_remote_copy(
            src_ref=w_ref if j == 0 else wbuf.at[slab(owner)],
            dst_ref=wbuf.at[slab(owner)],
            send_sem=f_send.at[j],
            recv_sem=f_recv.at[j],
            device_id=(sibling, s),
            device_id_type=MESH,
        )

    for j in range(1, pairs):
        w_copy(j).start()
    f_copy(0).start()
    for h in range(2):
        for way in range(2):
            token_copy(way, 0, h).start()
    wbuf[slab(d), :] = w_ref[...]

    def process(block, owner):
        y = jnp.dot(block, wbuf[...], preferred_element_type=jnp.float32) + b_ref[...]
        y = y.astype(jnp.bfloat16)
        at = pl.ds(pl.multiple_of(owner * tok, 16), tok)
        for i in range(images):
            out_ref[i, at, :] = y[i * tok : (i + 1) * tok]

    for t in range(steps):
        last = t == steps - 1
        for h in range(2):
            for way in range(2):
                if last and h != way:
                    continue
                token_copy(way, t, h, True).wait_recv()
                if t < steps - 2 or (t == steps - 2 and h == way):
                    token_copy(way, t + 1, h).start()
        if t == 0:
            for j in range(1, pairs):
                w_copy(j, True).wait_recv()
                f_copy(j).start()
            for j in range(pairs):
                f_copy(j, True).wait_recv()
            process(x_ref[...], s)
        if last:
            far = (place + n // 2) % n
            process(buf[far], ring_to_seq(far, n))
        else:

            def both(i, carry):
                origin = (place + n - (t + 1) + i * 2 * (t + 1)) % n
                process(buf[origin], ring_to_seq(origin, n))
                return carry

            lax.fori_loop(0, 2, both, 0)

    for j in range(1, pairs):
        w_copy(j).wait_send()
    for j in range(pairs):
        f_copy(j).wait_send()
    for t in range(steps):
        for h in range(2):
            for way in range(2):
                if t < steps - 1 or h == way:
                    token_copy(way, t, h).wait_send()


def project(normed, w_cols, bias, images, n, n_dp):
    rows, width = normed.shape
    depth, columns = w_cols.shape
    length = n * (rows // images)
    pairs = n_dp // 2
    dma = pltpu.SemaphoreType.DMA
    return pl.pallas_call(
        functools.partial(project_kernel, n, n_dp),
        out_shape=jax.ShapeDtypeStruct((images, length, columns), jnp.bfloat16),
        in_specs=[VMEM] * 3,
        out_specs=VMEM,
        scratch_shapes=[
            pltpu.VMEM((n, rows, width), jnp.bfloat16),
            pltpu.VMEM((width, columns), jnp.bfloat16),
            dma((2, n // 2, 2)),
            dma((2, n // 2, 2)),
            dma((pairs,)),
            dma((pairs,)),
            dma((pairs,)),
            dma((pairs,)),
        ],
        compiler_params=pltpu.CompilerParams(
            collective_id=0, has_side_effects=True, vmem_limit_bytes=40 * 1024 * 1024
        ),
        cost_estimate=pl.CostEstimate(
            flops=100 * 2 * n * rows * width * columns, bytes_accessed=n * rows * width * 2, transcendentals=0
        ),
        name="gather_project",
    )(normed, w_cols, bias)


def attend_kernel(heads, head_size, factor, packed_ref, out_ref):
    block_rows = out_ref.shape[0]
    at = pl.ds(pl.multiple_of(pl.program_id(1) * block_rows, 16), block_rows)
    mixed = []
    for h in range(heads):
        base = h * 3 * LANES
        queries = packed_ref[at, base : base + LANES]
        key_rows = packed_ref[:, base + LANES : base + 2 * LANES]
        value_rows = packed_ref[:, base + 2 * LANES : base + 3 * LANES]
        scores = lax.dot_general(
            queries, key_rows, (((1,), (1,)), ((), ())), preferred_element_type=jnp.float32
        )
        highest = jnp.max(scores, axis=-1, keepdims=True)
        weights = jnp.exp2((scores - highest) * factor).astype(jnp.bfloat16)
        summed = jnp.dot(weights, value_rows, preferred_element_type=jnp.float32)
        mixed.append(summed[:, :head_size] / summed[:, head_size : head_size + 1])
    out_ref[...] = jnp.concatenate(mixed, axis=-1).astype(jnp.bfloat16)


def attend(packed, heads, head_size):
    images, length, columns = packed.shape
    block_rows = max(r for r in range(16, 385, 16) if length % r == 0)
    factor = math.log2(math.e) / math.sqrt(head_size)
    return pl.pallas_call(
        functools.partial(attend_kernel, heads, head_size, factor),
        grid=(images, length // block_rows),
        out_shape=jax.ShapeDtypeStruct((images, length, heads * head_size), jnp.bfloat16),
        in_specs=[pl.BlockSpec((None, length, columns), lambda i, q: (i, 0, 0))],
        out_specs=pl.BlockSpec((None, block_rows, heads * head_size), lambda i, q: (i, q, 0)),
        compiler_params=pltpu.CompilerParams(vmem_limit_bytes=40 * 1024 * 1024),
        cost_estimate=pl.CostEstimate(
            flops=20 * images * heads * length * length * LANES,
            bytes_accessed=images * length * columns * 2,
            transcendentals=images * heads * length * length,
        ),
        name="attend",
    )(packed)


def exchange_kernel(n, ctx_ref, out_ref, send, recv):
    d, s = lax.axis_index("dp"), lax.axis_index("seq")
    tok = out_ref.shape[2]
    barrier = pltpu.get_barrier_semaphore()
    for t in range(1, n):
        pl.semaphore_signal(barrier, inc=1, device_id=(d, (s + t) % n), device_id_type=MESH)
    pl.semaphore_wait(barrier, n - 1)

    def rows_of(owner):
        return pl.ds(pl.multiple_of(owner * tok, 16), tok)

    def block_copy(t, arriving=False):
        peer = (s + t) % n
        slot = (s + n - t) % n if arriving else s
        return pltpu.make_async_remote_copy(
            src_ref=ctx_ref.at[:, rows_of(peer), :],
            dst_ref=out_ref.at[slot],
            send_sem=send.at[t],
            recv_sem=recv.at[t],
            device_id=(d, peer),
            device_id_type=MESH,
        )

    for t in range(1, n):
        block_copy(t).start()
    out_ref[s] = ctx_ref[:, rows_of(s), :]
    for t in range(1, n):
        block_copy(t, True).wait_recv()
    for t in range(1, n):
        block_copy(t).wait_send()


def exchange(context, n):
    images, length, columns = context.shape
    dma = pltpu.SemaphoreType.DMA
    return pl.pallas_call(
        functools.partial(exchange_kernel, n),
        out_shape=jax.ShapeDtypeStruct((n, images, length // n, columns), jnp.bfloat16),
        in_specs=[VMEM],
        out_specs=VMEM,
        scratch_shapes=[dma((n,)), dma((n,))],
        compiler_params=pltpu.CompilerParams(
            collective_id=1, has_side_effects=True, vmem_limit_bytes=16 * 1024 * 1024
        ),
        cost_estimate=pl.CostEstimate(
            flops=20_000_000_000, bytes_accessed=2 * images * length * columns, transcendentals=0
        ),
        name="exchange_context",
    )(context)


def head_columns(array, s, heads, head_size):
    span = heads * 3 * head_size
    mine = lax.dynamic_slice_in_dim(array, s * span, span, axis=1)
    mine = mine.reshape(array.shape[0], heads, 3, head_size)
    return jnp.pad(mine, ((0, 0), (0, 0), (0, 0), (0, LANES - head_size)))


def shards(
    n,
    n_dp,
    tokens,
    pre_gain,
    pre_shift,
    w_qkv,
    qkv_bias,
    w_out,
    out_bias,
    mlp_gain,
    mlp_shift,
    w_up,
    up_bias,
    w_down,
    down_bias,
):
    images_here, tok_here, width = tokens.shape
    row_count = images_here * tok_here
    heads_here = HEADS // n
    columns = heads_here * 3 * LANES
    s = lax.axis_index("seq")
    residual = tokens.reshape(row_count, width).astype(jnp.float32)
    normed = normalize(residual, pre_gain, pre_shift).astype(jnp.bfloat16)
    w_cols = head_columns(w_qkv, s, heads_here, HEAD_DIM).reshape(w_qkv.shape[0], columns)
    bias = head_columns(qkv_bias[None], s, heads_here, HEAD_DIM)
    bias = bias.at[:, :, 2, HEAD_DIM].set(1.0).reshape(1, columns)
    packed = project(normed, w_cols, bias, images_here, n, n_dp)
    context = attend(packed, heads_here, HEAD_DIM)
    context = exchange(context, n)
    context = context.transpose(1, 2, 0, 3).reshape(row_count, width)
    attended = fold_rows(context, lax.all_gather(w_out, "dp", axis=0, tiled=True))
    middle = residual + attended + out_bias
    normed_mlp = normalize(middle, mlp_gain, mlp_shift).astype(jnp.bfloat16)
    lifted = fold_rows(normed_mlp, lax.all_gather(w_up, "dp", axis=0, tiled=True))
    hidden = jax.nn.gelu(lifted + up_bias, approximate=False).astype(jnp.bfloat16)
    lowered = fold_rows(hidden, lax.all_gather(w_down, "dp", axis=0, tiled=True))
    result = (middle + lowered + down_bias).astype(jnp.bfloat16)
    return result.reshape(images_here, tok_here, width)


def solution(mesh):
    in_specs = (
        P("dp", "seq", None),
        P(),
        P(),
        P("dp", None),
        P(),
        P("dp", None),
        P(),
        P(),
        P(),
        P("dp", None),
        P(),
        P("dp", None),
        P(),
    )
    out_specs = P("dp", "seq", None)
    step = functools.partial(shards, mesh.shape["seq"], mesh.shape["dp"])
    return jax.shard_map(step, mesh=mesh, in_specs=in_specs, out_specs=out_specs, check_vma=False)
```

```python
import functools
import math

import jax
import jax.numpy as jnp
from jax import lax
from jax.experimental import pallas as pl
from jax.experimental.pallas import tpu as pltpu
from jax.sharding import PartitionSpec as P

HEADS = 16
HEAD_DIM = 80
LANES = 128
EPSILON = 1e-05
MESH = pl.DeviceIdType.MESH
VMEM = pl.BlockSpec(memory_space=pltpu.VMEM)


def normalize(features, gain, shift):
    average = jnp.mean(features, axis=-1, keepdims=True)
    centered = features - average
    spread = jnp.mean(centered * centered, axis=-1, keepdims=True)
    return centered * lax.rsqrt(spread + EPSILON) * gain + shift


def fold_rows(left_side, shard_piece):
    return jnp.dot(left_side, shard_piece, preferred_element_type=jnp.float32)


def ring_to_seq(place, n):
    back = place // (n // 2)
    return (1 - back) * 2 * place + back * (2 * (n - 1 - place) + 1)


def seq_to_ring(s, n):
    odd = s % 2
    return (1 - odd) * (s // 2) + odd * (n - 1 - s // 2)


def layer_kernel(
    n,
    n_dp,
    heads,
    head_size,
    block_rows,
    x_ref,
    w_ref,
    b_ref,
    out_shard,
    up_shard,
    down_shard,
    ctx_ref,
    out_full,
    up_full,
    down_full,
    buf,
    wbuf,
    packed,
    mixed,
    landed,
    tok_send,
    tok_recv,
    w_send,
    w_recv,
    f_send,
    f_recv,
    own_sem,
    c_send,
    c_recv,
):
    d, s = lax.axis_index("dp"), lax.axis_index("seq")
    place = seq_to_ring(s, n)
    right = ring_to_seq((place + 1) % n, n)
    left = ring_to_seq((place + n - 1) % n, n)
    sibling = d + 1 - 2 * (d % 2)
    half = x_ref.shape[0] // 2
    images, length, _ = packed.shape
    tok = length // n
    steps = n // 2
    pairs = n_dp // 2
    span = heads * head_size
    shards_of = (w_ref, out_shard, up_shard, down_shard)
    wholes = (wbuf, out_full, up_full, down_full)
    factor = math.log2(math.e) / math.sqrt(head_size)

    barrier = pltpu.get_barrier_semaphore()
    for t in range(1, n):
        pl.semaphore_signal(barrier, inc=1, device_id=(d, (s + t) % n), device_id_type=MESH)
    for j in range(1, pairs):
        pl.semaphore_signal(barrier, inc=1, device_id=((d + 2 * j) % n_dp, s), device_id_type=MESH)
    pl.semaphore_signal(barrier, inc=1, device_id=(sibling, s), device_id_type=MESH)
    pl.semaphore_wait(barrier, n - 1 + pairs)

    def token_copy(way, t, h, arriving=False):
        back = t + 1 if arriving else t
        origin = (place + n - back) % n if way == 0 else (place + back) % n
        part = pl.ds(h * half, half)
        here = buf.at[origin, part]
        return pltpu.make_async_remote_copy(
            src_ref=x_ref.at[part] if (t == 0 and not arriving) else here,
            dst_ref=here,
            send_sem=tok_send.at[way, t, h],
            recv_sem=tok_recv.at[way, t, h],
            device_id=(d, right if way == 0 else left),
            device_id_type=MESH,
        )

    def slab(k, owner):
        depth = shards_of[k].shape[0]
        return pl.ds(pl.multiple_of(owner * depth, 16), depth)

    def w_copy(k, j, arriving=False):
        owner = (d + n_dp - 2 * j) % n_dp if arriving else d
        return pltpu.make_async_remote_copy(
            src_ref=shards_of[k],
            dst_ref=wholes[k].at[slab(k, owner)],
            send_sem=w_send.at[k, j],
            recv_sem=w_recv.at[k, j],
            device_id=((d + 2 * j) % n_dp, s),
            device_id_type=MESH,
        )

    def f_copy(k, j, arriving=False):
        base = sibling if arriving else d
        owner = (base + n_dp - 2 * j) % n_dp
        there = wholes[k].at[slab(k, owner)]
        return pltpu.make_async_remote_copy(
            src_ref=shards_of[k] if j == 0 else there,
            dst_ref=there,
            send_sem=f_send.at[k, j],
            recv_sem=f_recv.at[k, j],
            device_id=(sibling, s),
            device_id_type=MESH,
        )

    def pass_on(k):
        for j in range(1, pairs):
            w_copy(k, j, True).wait_recv()
            f_copy(k, j).start()

    def own_copy(k):
        return pltpu.make_async_copy(shards_of[k], wholes[k].at[slab(k, d)], own_sem.at[k])

    def rows_of(owner):
        return pl.ds(pl.multiple_of(owner * tok, 16), tok)

    def ctx_copy(i, t, arriving=False):
        peer = (s + t) % n
        slot = (s + n - t) % n if arriving else s
        return pltpu.make_async_remote_copy(
            src_ref=mixed.at[i, rows_of(peer), :],
            dst_ref=landed.at[slot, i],
            send_sem=c_send.at[i, t],
            recv_sem=c_recv.at[i, t],
            device_id=(d, peer),
            device_id_type=MESH,
        )

    for j in range(1, pairs):
        w_copy(0, j).start()
    f_copy(0, 0).start()
    for h in range(2):
        for way in range(2):
            token_copy(way, 0, h).start()
    for k in range(1, 4):
        for j in range(1, pairs):
            w_copy(k, j).start()
        f_copy(k, 0).start()
        own_copy(k).start()
    wbuf[slab(0, d), :] = w_ref[...]

    def process(block, owner):
        y = jnp.dot(block, wbuf[...], preferred_element_type=jnp.float32) + b_ref[...]
        y = y.astype(jnp.bfloat16)
        for i in range(images):
            packed[i, rows_of(owner), :] = y[i * tok : (i + 1) * tok]

    for t in range(steps):
        last = t == steps - 1
        for h in range(2):
            for way in range(2):
                if last and h != way:
                    continue
                token_copy(way, t, h, True).wait_recv()
                if t < steps - 2 or (t == steps - 2 and h == way):
                    token_copy(way, t + 1, h).start()
        if t == 0:
            pass_on(0)
            for j in range(pairs):
                f_copy(0, j, True).wait_recv()
            process(x_ref[...], s)
        if last:
            pass_on(1)
            far = (place + n // 2) % n
            process(buf[far], ring_to_seq(far, n))
        else:

            def both(i, carry):
                origin = (place + n - (t + 1) + i * 2 * (t + 1)) % n
                process(buf[origin], ring_to_seq(origin, n))
                return carry

            lax.fori_loop(0, 2, both, 0)

    def attend_image(i, carry):
        def attend_block(block, inner):
            at = pl.ds(pl.multiple_of(block * block_rows, 16), block_rows)
            parts = []
            for h in range(heads):
                base = h * 3 * LANES
                queries = packed[i, at, base : base + LANES]
                key_rows = packed[i, :, base + LANES : base + 2 * LANES]
                value_rows = packed[i, :, base + 2 * LANES : base + 3 * LANES]
                scores = lax.dot_general(
                    queries, key_rows, (((1,), (1,)), ((), ())), preferred_element_type=jnp.float32
                )
                highest = jnp.max(scores, axis=-1, keepdims=True)
                weights = jnp.exp2((scores - highest) * factor).astype(jnp.bfloat16)
                summed = jnp.dot(weights, value_rows, preferred_element_type=jnp.float32)
                parts.append(summed[:, :head_size] / summed[:, head_size : head_size + 1])
            mixed[i, at, :] = jnp.concatenate(parts, axis=-1).astype(jnp.bfloat16)
            return inner

        lax.fori_loop(0, length // block_rows, attend_block, 0)
        landed[s, i] = mixed[i, rows_of(s), :]
        for t in range(1, n):
            ctx_copy(i, t).start()
        return carry

    lax.fori_loop(0, images, attend_image, 0)
    pass_on(2)

    def gather_image(i, carry):
        for t in range(1, n):
            ctx_copy(i, t, True).wait_recv()
        rows = pl.ds(pl.multiple_of(i * tok, 16), tok)
        for owner in range(n):
            ctx_ref[rows, owner * span : (owner + 1) * span] = landed[owner, i]
        return carry

    lax.fori_loop(0, images, gather_image, 0)
    pass_on(3)

    for k in range(4):
        for j in range(pairs):
            if k > 0:
                f_copy(k, j, True).wait_recv()
            if j > 0:
                w_copy(k, j).wait_send()
            f_copy(k, j).wait_send()
        if k > 0:
            own_copy(k).wait()
    for t in range(steps):
        for h in range(2):
            for way in range(2):
                if t < steps - 1 or h == way:
                    token_copy(way, t, h).wait_send()
    for i in range(images):
        for t in range(1, n):
            ctx_copy(i, t).wait_send()


def attention_and_weights(normed, w_cols, bias, w_out, w_up, w_down, images, heads, n, n_dp):
    rows, width = normed.shape
    columns = w_cols.shape[1]
    tok = rows // images
    length = n * tok
    pairs = n_dp // 2
    span = heads * HEAD_DIM
    block_rows = max(r for r in range(16, 385, 16) if length % r == 0)
    dma = pltpu.SemaphoreType.DMA
    half = jnp.bfloat16
    anywhere = pl.BlockSpec(memory_space=pl.ANY)

    def full(shard):
        return jax.ShapeDtypeStruct((n_dp * shard.shape[0], shard.shape[1]), half)

    return pl.pallas_call(
        functools.partial(layer_kernel, n, n_dp, heads, HEAD_DIM, block_rows),
        out_shape=(jax.ShapeDtypeStruct((rows, n * span), half), full(w_out), full(w_up), full(w_down)),
        in_specs=[VMEM] * 6,
        out_specs=(VMEM, anywhere, anywhere, anywhere),
        scratch_shapes=[
            pltpu.VMEM((n, rows, width), half),
            pltpu.VMEM((width, columns), half),
            pltpu.VMEM((images, length, columns), half),
            pltpu.VMEM((images, length, span), half),
            pltpu.VMEM((n, images, tok, span), half),
            dma((2, n // 2, 2)),
            dma((2, n // 2, 2)),
            dma((4, pairs)),
            dma((4, pairs)),
            dma((4, pairs)),
            dma((4, pairs)),
            dma((4,)),
            dma((images, n)),
            dma((images, n)),
        ],
        compiler_params=pltpu.CompilerParams(
            collective_id=0, has_side_effects=True, vmem_limit_bytes=56 * 1024 * 1024
        ),
        name="attention_and_weights",
    )(normed, w_cols, bias, w_out, w_up, w_down)


def head_columns(array, s, heads, head_size):
    span = heads * 3 * head_size
    mine = lax.dynamic_slice_in_dim(array, s * span, span, axis=1)
    mine = mine.reshape(array.shape[0], heads, 3, head_size)
    return jnp.pad(mine, ((0, 0), (0, 0), (0, 0), (0, LANES - head_size)))


def shards(
    n,
    n_dp,
    tokens,
    pre_gain,
    pre_shift,
    w_qkv,
    qkv_bias,
    w_out,
    out_bias,
    mlp_gain,
    mlp_shift,
    w_up,
    up_bias,
    w_down,
    down_bias,
):
    images_here, tok_here, width = tokens.shape
    row_count = images_here * tok_here
    heads_here = HEADS // n
    columns = heads_here * 3 * LANES
    s = lax.axis_index("seq")
    residual = tokens.reshape(row_count, width).astype(jnp.float32)
    normed = normalize(residual, pre_gain, pre_shift).astype(jnp.bfloat16)
    w_cols = head_columns(w_qkv, s, heads_here, HEAD_DIM).reshape(w_qkv.shape[0], columns)
    bias = head_columns(qkv_bias[None], s, heads_here, HEAD_DIM)
    bias = bias.at[:, :, 2, HEAD_DIM].set(1.0).reshape(1, columns)
    context, w_out, w_up, w_down = attention_and_weights(
        normed, w_cols, bias, w_out, w_up, w_down, images_here, heads_here, n, n_dp
    )
    attended = fold_rows(context, w_out)
    middle = residual + attended + out_bias
    normed_mlp = normalize(middle, mlp_gain, mlp_shift).astype(jnp.bfloat16)
    lifted = fold_rows(normed_mlp, w_up)
    hidden = jax.nn.gelu(lifted + up_bias, approximate=False).astype(jnp.bfloat16)
    lowered = fold_rows(hidden, w_down)
    result = (middle + lowered + down_bias).astype(jnp.bfloat16)
    return result.reshape(images_here, tok_here, width)


def solution(mesh):
    in_specs = (
        P("dp", "seq", None),
        P(),
        P(),
        P("dp", None),
        P(),
        P("dp", None),
        P(),
        P(),
        P(),
        P("dp", None),
        P(),
        P("dp", None),
        P(),
    )
    out_specs = P("dp", "seq", None)
    step = functools.partial(shards, mesh.shape["seq"], mesh.shape["dp"])
    return jax.shard_map(step, mesh=mesh, in_specs=in_specs, out_specs=out_specs, check_vma=False)
```

```python
import functools
import math

import jax
import jax.numpy as jnp
from jax import lax
from jax.experimental import pallas as pl
from jax.experimental.pallas import tpu as pltpu
from jax.sharding import PartitionSpec as P

HEADS = 16
HEAD_DIM = 80
LANES = 128
EPSILON = 1e-05
MESH = pl.DeviceIdType.MESH
VMEM = pl.BlockSpec(memory_space=pltpu.VMEM)


def normalize(features, gain, shift):
    average = jnp.mean(features, axis=-1, keepdims=True)
    centered = features - average
    spread = jnp.mean(centered * centered, axis=-1, keepdims=True)
    return centered * lax.rsqrt(spread + EPSILON) * gain + shift


def fold_rows(left_side, shard_piece):
    return jnp.dot(left_side, shard_piece, preferred_element_type=jnp.float32)


def ring_to_seq(place, n):
    back = place // (n // 2)
    return (1 - back) * 2 * place + back * (2 * (n - 1 - place) + 1)


def seq_to_ring(s, n):
    odd = s % 2
    return (1 - odd) * (s // 2) + odd * (n - 1 - s // 2)


def layer_kernel(
    n,
    n_dp,
    heads,
    head_size,
    block_rows,
    x_ref,
    w_ref,
    b_ref,
    out_shard,
    up_shard,
    down_shard,
    tok_ref,
    ob_ref,
    gain_ref,
    shift_ref,
    ub_ref,
    middle_ref,
    hidden_ref,
    down_full,
    out_full,
    up_full,
    ctx_ref,
    buf,
    wraw,
    wbuf,
    packed,
    mixed,
    landed,
    tok_send,
    tok_recv,
    w_send,
    w_recv,
    f_send,
    f_recv,
    own_sem,
    c_send,
    c_recv,
):
    d, s = lax.axis_index("dp"), lax.axis_index("seq")
    place = seq_to_ring(s, n)
    right = ring_to_seq((place + 1) % n, n)
    left = ring_to_seq((place + n - 1) % n, n)
    sibling = d + 1 - 2 * (d % 2)
    half = x_ref.shape[0] // 2
    images, length, _ = packed.shape
    tok = length // n
    steps = n // 2
    pairs = n_dp // 2
    span = heads * head_size
    shards_of = (w_ref, out_shard, up_shard, down_shard)
    wholes = (wraw, out_full, up_full, down_full)
    factor = math.log2(math.e) / math.sqrt(head_size)

    barrier = pltpu.get_barrier_semaphore()
    for t in range(1, n):
        pl.semaphore_signal(barrier, inc=1, device_id=(d, (s + t) % n), device_id_type=MESH)
    for j in range(1, pairs):
        pl.semaphore_signal(barrier, inc=1, device_id=((d + 2 * j) % n_dp, s), device_id_type=MESH)
    pl.semaphore_signal(barrier, inc=1, device_id=(sibling, s), device_id_type=MESH)
    pl.semaphore_wait(barrier, n - 1 + pairs)

    def token_copy(way, t, h, arriving=False):
        back = t + 1 if arriving else t
        origin = (place + n - back) % n if way == 0 else (place + back) % n
        part = pl.ds(h * half, half)
        here = buf.at[origin, part]
        return pltpu.make_async_remote_copy(
            src_ref=x_ref.at[part] if (t == 0 and not arriving) else here,
            dst_ref=here,
            send_sem=tok_send.at[way, t, h],
            recv_sem=tok_recv.at[way, t, h],
            device_id=(d, right if way == 0 else left),
            device_id_type=MESH,
        )

    def slab(k, owner):
        depth = shards_of[k].shape[0]
        return pl.ds(pl.multiple_of(owner * depth, 16), depth)

    def w_copy(k, j, arriving=False):
        owner = (d + n_dp - 2 * j) % n_dp if arriving else d
        return pltpu.make_async_remote_copy(
            src_ref=shards_of[k],
            dst_ref=wholes[k].at[slab(k, owner)],
            send_sem=w_send.at[k, j],
            recv_sem=w_recv.at[k, j],
            device_id=((d + 2 * j) % n_dp, s),
            device_id_type=MESH,
        )

    def f_copy(k, j, arriving=False):
        base = sibling if arriving else d
        owner = (base + n_dp - 2 * j) % n_dp
        there = wholes[k].at[slab(k, owner)]
        return pltpu.make_async_remote_copy(
            src_ref=shards_of[k] if j == 0 else there,
            dst_ref=there,
            send_sem=f_send.at[k, j],
            recv_sem=f_recv.at[k, j],
            device_id=(sibling, s),
            device_id_type=MESH,
        )

    def pass_on(k):
        for j in range(1, pairs):
            w_copy(k, j, True).wait_recv()
            f_copy(k, j).start()

    def own_copy(k):
        return pltpu.make_async_copy(shards_of[k], wholes[k].at[slab(k, d)], own_sem.at[k])

    def rows_of(owner):
        return pl.ds(pl.multiple_of(owner * tok, 16), tok)

    def ctx_copy(i, t, arriving=False):
        peer = (s + t) % n
        slot = (s + n - t) % n if arriving else s
        return pltpu.make_async_remote_copy(
            src_ref=mixed.at[i, rows_of(peer), :],
            dst_ref=landed.at[slot, i],
            send_sem=c_send.at[i, t],
            recv_sem=c_recv.at[i, t],
            device_id=(d, peer),
            device_id_type=MESH,
        )

    for j in range(1, pairs):
        w_copy(0, j).start()
    f_copy(0, 0).start()
    for h in range(2):
        for way in range(2):
            token_copy(way, 0, h).start()
    for k in range(1, 4):
        for j in range(1, pairs):
            w_copy(k, j).start()
        f_copy(k, 0).start()
    own_copy(3).start()
    for k in range(3):
        wholes[k][slab(k, d), :] = shards_of[k][...]

    def process(block, owner):
        y = jnp.dot(block, wbuf[...], preferred_element_type=jnp.float32) + b_ref[...]
        y = y.astype(jnp.bfloat16)
        for i in range(images):
            packed[i, rows_of(owner), :] = y[i * tok : (i + 1) * tok]

    for t in range(steps):
        last = t == steps - 1
        for h in range(2):
            for way in range(2):
                if last and h != way:
                    continue
                token_copy(way, t, h, True).wait_recv()
                if t < steps - 2 or (t == steps - 2 and h == way):
                    token_copy(way, t + 1, h).start()
        if t == 0:
            pass_on(0)
            for j in range(pairs):
                f_copy(0, j, True).wait_recv()
            wbuf[...] = jnp.zeros_like(wbuf)
            for g in range(3 * heads):
                wbuf[:, g * LANES : g * LANES + head_size] = wraw[:, g * head_size : (g + 1) * head_size]
            process(x_ref[...], s)
        if last:
            pass_on(1)
            far = (place + n // 2) % n
            process(buf[far], ring_to_seq(far, n))
        else:

            def both(i, carry):
                origin = (place + n - (t + 1) + i * 2 * (t + 1)) % n
                process(buf[origin], ring_to_seq(origin, n))
                return carry

            lax.fori_loop(0, 2, both, 0)

    def attend_image(i, carry):
        def attend_block(block, inner):
            at = pl.ds(pl.multiple_of(block * block_rows, 16), block_rows)
            parts = []
            for h in range(heads):
                base = h * 3 * LANES
                queries = packed[i, at, base : base + LANES]
                key_rows = packed[i, :, base + LANES : base + 2 * LANES]
                value_rows = packed[i, :, base + 2 * LANES : base + 3 * LANES]
                scores = lax.dot_general(
                    queries, key_rows, (((1,), (1,)), ((), ())), preferred_element_type=jnp.float32
                )
                highest = jnp.max(scores, axis=-1, keepdims=True)
                weights = jnp.exp2((scores - highest) * factor).astype(jnp.bfloat16)
                summed = jnp.dot(weights, value_rows, preferred_element_type=jnp.float32)
                parts.append(summed[:, :head_size] / summed[:, head_size : head_size + 1])
            mixed[i, at, :] = jnp.concatenate(parts, axis=-1).astype(jnp.bfloat16)
            return inner

        lax.fori_loop(0, length // block_rows, attend_block, 0)
        landed[s, i] = mixed[i, rows_of(s), :]
        for t in range(1, n):
            ctx_copy(i, t).start()
        return carry

    lax.fori_loop(0, images, attend_image, 0)
    pass_on(2)

    def gather_image(i, carry):
        for t in range(1, n):
            ctx_copy(i, t, True).wait_recv()
        rows = pl.ds(pl.multiple_of(i * tok, 16), tok)
        for owner in range(n):
            ctx_ref[rows, owner * span : (owner + 1) * span] = landed[owner, i]
        return carry

    for k in range(1, 3):
        for j in range(pairs):
            f_copy(k, j, True).wait_recv()
    lax.fori_loop(0, images, gather_image, 0)

    def tile_of(c):
        return pl.ds(pl.multiple_of(c * 2 * LANES, 2 * LANES), 2 * LANES)

    def out_tile(c, carry):
        cols = tile_of(c)
        attended = jnp.dot(ctx_ref[...], out_full[:, cols], preferred_element_type=jnp.float32)
        middle_ref[:, cols] = tok_ref[:, cols].astype(jnp.float32) + attended + ob_ref[:, cols]
        return carry

    def up_tile(c, carry):
        cols = tile_of(c)
        lifted = jnp.dot(ctx_ref[...], up_full[:, cols], preferred_element_type=jnp.float32)
        lifted = lifted + ub_ref[:, cols]
        hidden = 0.5 * lifted * (1.0 + lax.erf(lifted * math.sqrt(0.5)))
        hidden_ref[:, cols] = hidden.astype(jnp.bfloat16)
        return carry

    lax.fori_loop(0, out_full.shape[1] // (2 * LANES), out_tile, 0)
    ctx_ref[...] = normalize(middle_ref[...], gain_ref[...], shift_ref[...]).astype(jnp.bfloat16)
    lax.fori_loop(0, up_full.shape[1] // (2 * LANES), up_tile, 0)
    pass_on(3)

    for k in range(4):
        for j in range(pairs):
            if k == 3:
                f_copy(k, j, True).wait_recv()
            if j > 0:
                w_copy(k, j).wait_send()
            f_copy(k, j).wait_send()
    own_copy(3).wait()
    for t in range(steps):
        for h in range(2):
            for way in range(2):
                if t < steps - 1 or h == way:
                    token_copy(way, t, h).wait_send()
    for i in range(images):
        for t in range(1, n):
            ctx_copy(i, t).wait_send()


def layer_until_hidden(
    normed, w_cols, bias, w_out, w_up, w_down, tokens, out_bias, gain, shift, up_bias, images, heads, n, n_dp
):
    rows, width = normed.shape
    columns = 3 * heads * LANES
    tok = rows // images
    length = n * tok
    pairs = n_dp // 2
    span = heads * HEAD_DIM
    block_rows = max(r for r in range(16, 385, 16) if length % r == 0)
    dma = pltpu.SemaphoreType.DMA
    half = jnp.bfloat16
    anywhere = pl.BlockSpec(memory_space=pl.ANY)

    def full(shard):
        return (n_dp * shard.shape[0], shard.shape[1])

    return pl.pallas_call(
        functools.partial(layer_kernel, n, n_dp, heads, HEAD_DIM, block_rows),
        out_shape=(
            jax.ShapeDtypeStruct((rows, width), jnp.float32),
            jax.ShapeDtypeStruct((rows, w_up.shape[1]), half),
            jax.ShapeDtypeStruct(full(w_down), half),
        ),
        in_specs=[VMEM] * 11,
        out_specs=(VMEM, VMEM, anywhere),
        scratch_shapes=[
            pltpu.VMEM(full(w_out), half),
            pltpu.VMEM(full(w_up), half),
            pltpu.VMEM((rows, n * span), half),
            pltpu.VMEM((n, rows, width), half),
            pltpu.VMEM(full(w_cols), half),
            pltpu.VMEM((width, columns), half),
            pltpu.VMEM((images, length, columns), half),
            pltpu.VMEM((images, length, span), half),
            pltpu.VMEM((n, images, tok, span), half),
            dma((2, n // 2, 2)),
            dma((2, n // 2, 2)),
            dma((4, pairs)),
            dma((4, pairs)),
            dma((4, pairs)),
            dma((4, pairs)),
            dma((4,)),
            dma((images, n)),
            dma((images, n)),
        ],
        compiler_params=pltpu.CompilerParams(
            collective_id=0, has_side_effects=True, vmem_limit_bytes=56 * 1024 * 1024
        ),
        name="layer_until_hidden",
    )(normed, w_cols, bias, w_out, w_up, w_down, tokens, out_bias, gain, shift, up_bias)


def head_columns(array, s, heads, head_size):
    span = heads * 3 * head_size
    mine = lax.dynamic_slice_in_dim(array, s * span, span, axis=1)
    mine = mine.reshape(array.shape[0], heads, 3, head_size)
    return jnp.pad(mine, ((0, 0), (0, 0), (0, 0), (0, LANES - head_size)))


def shards(
    n,
    n_dp,
    tokens,
    pre_gain,
    pre_shift,
    w_qkv,
    qkv_bias,
    w_out,
    out_bias,
    mlp_gain,
    mlp_shift,
    w_up,
    up_bias,
    w_down,
    down_bias,
):
    images_here, tok_here, width = tokens.shape
    row_count = images_here * tok_here
    heads_here = HEADS // n
    columns = heads_here * 3 * LANES
    s = lax.axis_index("seq")
    residual = tokens.reshape(row_count, width).astype(jnp.float32)
    normed = normalize(residual, pre_gain, pre_shift).astype(jnp.bfloat16)
    span = heads_here * 3 * HEAD_DIM
    w_cols = lax.dynamic_slice_in_dim(w_qkv, s * span, span, axis=1)
    bias = head_columns(qkv_bias[None], s, heads_here, HEAD_DIM)
    bias = bias.at[:, :, 2, HEAD_DIM].set(1.0).reshape(1, columns)
    middle, hidden, w_down = layer_until_hidden(
        normed,
        w_cols,
        bias,
        w_out,
        w_up,
        w_down,
        tokens.reshape(row_count, width),
        out_bias[None],
        mlp_gain[None],
        mlp_shift[None],
        up_bias[None],
        images_here,
        heads_here,
        n,
        n_dp,
    )
    lowered = fold_rows(hidden, w_down)
    result = (middle + lowered + down_bias).astype(jnp.bfloat16)
    return result.reshape(images_here, tok_here, width)


def solution(mesh):
    in_specs = (
        P("dp", "seq", None),
        P(),
        P(),
        P("dp", None),
        P(),
        P("dp", None),
        P(),
        P(),
        P(),
        P("dp", None),
        P(),
        P("dp", None),
        P(),
    )
    out_specs = P("dp", "seq", None)
    step = functools.partial(shards, mesh.shape["seq"], mesh.shape["dp"])
    return jax.shard_map(step, mesh=mesh, in_specs=in_specs, out_specs=out_specs, check_vma=False)
```
